256 devices in a mesh: dp: 16 (over y, z_lo), tensor: 16 (over z_hi, x, core).
Axes of the slice: x: 4, y: 4, z: 8 (z_hi: 2, z_lo: 4; z = z_hi * 4 + z_lo), core: 2. Of those that a mesh axis runs over, the one named last changes fastest.
Arguments:
- cotangent: bfloat16 [4096, 8192], P(('dp', 'tensor')), may hold values from -0.78125 to 0.78125
- gate_pre: bfloat16 [4096, 14336], P('dp', 'tensor'), may hold values from -5 to 5
- up_pre: bfloat16 [4096, 14336], P('dp', 'tensor'), may hold values from -28 to 28
- row_state: float32 [8192], P('dp'), may hold values from 0.02 to 3
- column_state: float32 [14336], P('tensor'), may hold values from 0.05 to 2
Outputs:
- update: float32 [8192, 14336], P('dp', 'tensor')
- row_next: float32 [8192], P('dp')
- column_next: float32 [14336], P('tensor')
- row_scale: float32 [1], replicated
The draws below stay inside these ranges and needn't reach their ends.
All inputs are finite; a program needn't handle non-finite values.
Results may differ from the reference program's by a relative error of at most 0.019.
Values may be sent and summed in bfloat16 or wider, within the bound.
No kernel may reach another device: no remote copies, remote signals or barrier semaphores. Data moves between devices by JAX's collectives and lax.ppermute only.
A program may use at most 128 MiB of HBM per device.

```python
import math
import jax
import jax.numpy as jnp
from jax import lax

D = 8192
FF = 14336
TOK_DP = 256
TOKENS = 4096
N_DP = 16


def draw_cotangent(key, part):
    first_key, second_key = jax.random.split(key, 2)
    position = jnp.arange(D, dtype=jnp.float32) / D
    base = jnp.clip(jax.random.normal(first_key, (TOKENS, D), jnp.float32), -5.0, 5.0)
    spread = 10.0 ** (jax.random.uniform(second_key, (D,), jnp.float32) - 0.5)
    scale = spread * 3.0 ** (position - 0.5) / math.sqrt(TOKENS)
    return (base * scale[None, :]).astype(jnp.bfloat16)


def draw_up_pre(key, part):
    first_key, second_key = jax.random.split(key, 2)
    position = jnp.arange(FF, dtype=jnp.float32) / FF
    base = jnp.clip(jax.random.normal(first_key, (TOKENS, FF), jnp.float32), -5.0, 5.0)
    spread = 10.0 ** (jax.random.uniform(second_key, (FF,), jnp.float32) - 0.5)
    scale = spread * 3.0 ** (position - 0.5)
    return (base * scale[None, :]).astype(jnp.bfloat16)


def draw_row_state(key, part):
    position = jnp.arange(D, dtype=jnp.float32) / D
    level = jax.random.uniform(key, (D,), jnp.float32, 0.0, 1.0)
    return 0.02 * 10.0 ** (0.7 * level + 0.65 * position)


def shard_levels(key, shape, cuts, smallest, high):
    gain, own = 1.0, jax.random.fold_in(key, 6)
    for dim, parts in cuts:
        draws = jnp.exp(jax.random.uniform(jax.random.fold_in(own, dim), (parts,), jnp.float32, smallest / len(cuts), high / len(cuts)))
        gain = gain * jnp.repeat(draws, shape[dim] // parts).reshape([-1 if axis == dim else 1 for axis in range(len(shape))])
    return gain


def noise(stream_key, extent, width, most, cuts=(), kind=jnp.bfloat16):
    values = jax.random.normal(stream_key, extent, jnp.float32) * width
    if len(cuts) > 0:
        values = shard_levels(stream_key, extent, cuts, -0.22, 0.18) * values
    return jnp.clip(values, min=-most, max=most).astype(kind)


def setup_inputs(seed: int = 0) -> dict:
    keys = jax.random.split(jax.random.key(seed), 6)
    cotangent = draw_cotangent(jax.random.fold_in(keys[5], 71), 0)
    gate_pre = noise(keys[1], (TOKENS, FF), 1.0, 5.0, ((0, 16), (1, 16)))
    up_pre = draw_up_pre(jax.random.fold_in(keys[5], 71), 0)
    row_state = draw_row_state(jax.random.fold_in(keys[5], 71), 0)
    column_state = jnp.clip(jnp.exp(math.log(2.0) - 3.6888794 * jax.random.uniform(keys[4], (FF,), jnp.float32) ** shard_levels(keys[4], (FF,), ((0, 16),), -0.2, 0.2)), 0.05, 2.0)
    return {"cotangent": cotangent, "gate_pre": gate_pre, "up_pre": up_pre, "row_state": row_state, "column_state": column_state}


EPSILON = 1e-30
DECAY_RATE = 0.9

def reference(cotangent, gate_pre, up_pre, row_state, column_state):
    hidden = (jax.nn.silu(gate_pre.astype(jnp.float32)) * up_pre.astype(jnp.float32)).astype(jnp.bfloat16)
    cot_groups = cotangent.reshape(N_DP, TOK_DP, D)
    hid_groups = hidden.reshape(N_DP, TOK_DP, FF)

    def add_group(running, paired):
        partial_value = jnp.dot(paired[0].T, paired[1], preferred_element_type=jnp.float32)
        rounded = lax.optimization_barrier(partial_value.astype(jnp.bfloat16))
        return (running + rounded.astype(jnp.float32), None)
    gradient, _ = lax.scan(add_group, jnp.zeros((D, FF), jnp.float32), (cot_groups, hid_groups))
    squares = gradient * gradient + EPSILON
    row_next = DECAY_RATE * row_state + (1.0 - DECAY_RATE) * lax.optimization_barrier(jnp.mean(squares, axis=1))
    column_next = DECAY_RATE * column_state + (1.0 - DECAY_RATE) * lax.optimization_barrier(jnp.mean(squares, axis=0))
    row_mean = jnp.mean(row_next)
    second_moment = row_next[:, None] * column_next[None, :] / row_mean
    raw_update = gradient / jnp.sqrt(second_moment)
    norm_value = jnp.sqrt(jnp.mean(raw_update * raw_update))
    update = raw_update / jnp.maximum(1.0, norm_value)
    return (update, row_next, column_next, jnp.reshape(row_mean, (1,)))
```

```python
import functools

import jax
import jax.numpy as jnp
from jax import lax
from jax.experimental import pallas as pl
from jax.experimental.pallas import tpu as pltpu
from jax.sharding import Mesh
from jax.sharding import PartitionSpec as P

D = 8192
FF = 14336
Y, ZL, ZH, X, C = "y", "zl", "zh", "x", "c"
DP = (Y, ZL)
TENSOR = (ZH, X, C)
EPSILON = 1e-30
DECAY_RATE = 0.9
ROWS = 512
COLS = 896
TOK = 16
XS = (0, -1, 1, 2)
YS = (0, 1, -1, 2)

F32, BF16 = jnp.float32, jnp.bfloat16


def prepare_kernel(cot_ref, gate_ref, up_ref, pieces_ref, hidden_ref):
    y, zl, zh = lax.axis_index(Y), lax.axis_index(ZL), lax.axis_index(ZH)
    x, c = lax.axis_index(X), lax.axis_index(C)
    for d in range(4):
        for k in range(4):
            block = ((y + YS[k] + 4) % 4) * 4 + (zl + d) % 4
            start = pl.multiple_of(block * ROWS, ROWS)
            pieces_ref[d, :, k * ROWS : (k + 1) * ROWS] = cot_ref[:, pl.ds(start, ROWS)]
    for ci in range(2):
        for xi in range(4):
            for e in range(2):
                owner = ((zh + e) % 2) * 8 + ((x + XS[xi] + 4) % 4) * 2 + (c + ci) % 2
                start = pl.multiple_of(owner * TOK, TOK)
                gate = gate_ref[pl.ds(start, TOK), :].astype(F32)
                up = up_ref[pl.ds(start, TOK), :].astype(F32)
                at = ((ci * 4 + xi) * 2 + e) * TOK
                hidden_ref[at : at + TOK, :] = (gate / (1.0 + jnp.exp(-gate)) * up).astype(BF16)


def prepare(cot, gate, up):
    return pl.pallas_call(
        prepare_kernel,
        out_shape=(
            jax.ShapeDtypeStruct((4, TOK, 4 * ROWS), BF16),
            jax.ShapeDtypeStruct((256, COLS), BF16),
        ),
        cost_estimate=pl.CostEstimate(flops=2000000, bytes_accessed=2000000, transcendentals=0),
        compiler_params=pltpu.CompilerParams(vmem_limit_bytes=8 << 20),
        name="prepare",
    )(cot, gate, up)


def product(lhs_ref, cot_refs, hidden_ref, k):
    for i, ref in enumerate(cot_refs):
        lhs_ref[i * 128 : (i + 1) * 128, :] = ref[:, k * ROWS : (k + 1) * ROWS]
    return lax.dot_general(
        lhs_ref[...], hidden_ref[...], (((0,), (0,)), ((), ())), preferred_element_type=F32
    )


def far_kernel(*refs):
    cots, (h0, h1, h2a, h2b, h3), (top, bottom, hidden, lhs) = refs[:8], refs[8:13], refs[13:]
    for j in range(8):
        src = slice(j * 32, (j + 1) * 32)
        for d, ref in enumerate((h0, h1, None, h3)):
            value = h2a[src, :] + h2b[src, :] if d == 2 else ref[src, :]
            hidden[j * 128 + d * 32 : j * 128 + (d + 1) * 32, :] = value
    part = product(lhs, cots, hidden, 3).astype(BF16)
    top[...] = part[: ROWS // 2]
    bottom[...] = part[ROWS // 2 :]


def near_kernel(*refs):
    cots, hidden, (up_top, up_bottom, down_top, down_bottom, own, lhs) = refs[:8], refs[8], refs[9:]
    for k, (top, bottom) in ((1, (up_top, up_bottom)), (2, (down_top, down_bottom))):
        part = product(lhs, cots, hidden, k).astype(BF16)
        top[...] = part[: ROWS // 2]
        bottom[...] = part[ROWS // 2 :]
    own[...] = product(lhs, cots, hidden, 0)


HALF = jax.ShapeDtypeStruct((ROWS // 2, COLS), BF16)
ONE_PRODUCT = 2 * ROWS * COLS * 1024


def far(cots, hiddens):
    return pl.pallas_call(
        far_kernel,
        out_shape=(HALF, HALF, jax.ShapeDtypeStruct((1024, COLS), BF16)),
        scratch_shapes=[pltpu.VMEM((1024, ROWS), BF16)],
        cost_estimate=pl.CostEstimate(flops=ONE_PRODUCT, bytes_accessed=8000000, transcendentals=0),
        compiler_params=pltpu.CompilerParams(vmem_limit_bytes=24 << 20),
        name="far",
    )(*cots, *hiddens)


def near(cots, hidden):
    return pl.pallas_call(
        near_kernel,
        out_shape=(HALF, HALF, HALF, HALF, jax.ShapeDtypeStruct((ROWS, COLS), F32)),
        scratch_shapes=[pltpu.VMEM((1024, ROWS), BF16)],
        cost_estimate=pl.CostEstimate(flops=3 * ONE_PRODUCT, bytes_accessed=8000000, transcendentals=0),
        compiler_params=pltpu.CompilerParams(vmem_limit_bytes=24 << 20),
        name="near",
    )(*cots, hidden)


def ring(x, axis, step):
    return lax.ppermute(x, axis, [(i, (i + step) % 4) for i in range(4)])


def to_column(x, d, e):
    pairs = [(zl * 2 + zh, ((zl + d) % 4) * 2 + (zh + e) % 2) for zl in range(4) for zh in range(2)]
    return lax.ppermute(x, (ZL, ZH), pairs)


def from_everyone(x, axis):
    copies = jnp.broadcast_to(x, (lax.axis_size(axis), *x.shape))
    return lax.all_to_all(copies, axis, split_axis=0, concat_axis=0, tiled=True)


def shards(cotangent, gate_pre, up_pre, row_state, column_state):
    pieces, hidden = prepare(cotangent, gate_pre, up_pre)
    arrived = [
        pieces[0] if d == 0 and e == 0 else to_column(pieces[d], d, e) for d in range(4) for e in range(2)
    ]
    column = jnp.concatenate(arrived, axis=0)
    along_x = [column, ring(column, X, 1), ring(column, X, -1), ring(column, X, 2)]
    other_core = [lax.ppermute(v, C, [(0, 1), (1, 0)]) for v in along_x]
    cots = along_x + other_core
    below = ring(hidden, ZL, 1)
    above = ring(hidden, ZL, -1)
    far_up = lax.ppermute(below, ZL, [(1, 2), (2, 3)])
    far_down = lax.ppermute(above, ZL, [(2, 1), (1, 0)])
    far_top, far_bottom, all_hidden = far(cots, (hidden, below, far_up, far_down, above))
    got_top = ring(far_top, Y, 1)
    got_bottom = ring(far_bottom, Y, -1)
    up_top, up_bottom, down_top, down_bottom, own = near(cots, all_hidden)
    a_up = ring(up_bottom, Y, 1)
    a_down = ring(down_top, Y, -1)
    c_up = ring((up_top.astype(F32) + got_top.astype(F32)).astype(BF16), Y, 1)
    c_down = ring((down_bottom.astype(F32) + got_bottom.astype(F32)).astype(BF16), Y, -1)
    upper = own[: ROWS // 2] + (c_up.astype(F32) + a_down.astype(F32))
    lower = own[ROWS // 2 :] + (a_up.astype(F32) + c_down.astype(F32))
    gradient = jnp.concatenate([upper, lower], axis=0)

    squares = gradient * gradient + EPSILON
    column_part = jnp.sum(squares, axis=0)
    column_total = from_everyone(column_part, DP).sum(axis=0)
    column_next = DECAY_RATE * column_state + (1.0 - DECAY_RATE) * (column_total / D)
    row_part = jnp.sum(squares, axis=1)
    scaled_part = jnp.sum(gradient * gradient / column_next[None, :], axis=1)
    both = from_everyone(jnp.concatenate([row_part, scaled_part]), TENSOR).sum(axis=0)
    row_next = DECAY_RATE * row_state + (1.0 - DECAY_RATE) * (both[:ROWS] / FF)
    sums = jnp.stack([jnp.sum(row_next), jnp.sum(both[ROWS:] / row_next)])
    sums = from_everyone(sums, DP).sum(axis=0)
    row_mean = sums[0] / D
    norm_value = jnp.sqrt(row_mean * sums[1] / (float(D) * float(FF)))
    scale = jnp.sqrt(row_mean) / jnp.maximum(1.0, norm_value)
    update = gradient * lax.rsqrt(row_next)[:, None] * (lax.rsqrt(column_next) * scale)[None, :]
    return (update, row_next, column_next, jnp.reshape(row_mean, (1,)))


def solution(mesh):
    finer = Mesh(mesh.devices.reshape(4, 4, 2, 4, 2), (Y, ZL, ZH, X, C))
    placed = (P(DP + TENSOR, None), P(DP, TENSOR), P(DP, TENSOR), P(DP), P(TENSOR))
    return jax.shard_map(
        shards,
        mesh=finer,
        in_specs=placed,
        out_specs=(P(DP, TENSOR), P(DP), P(TENSOR), P()),
        check_vma=False,
    )
```
